32 devices in a mesh: grow: 4 (over y, x), gcol: 8 (over z, core).
Axes of the slice: x: 2, y: 2, z: 4, core: 2. Of those that a mesh axis runs over, the one named last changes fastest.
Arguments:
- psi: float32 [32768, 1024], P(('grow', 'gcol')), may hold values from -6 to 6
- vpsi: float32 [32768, 1024], P(('grow', 'gcol')), may hold values from -6 to 6
- kinetic: float32 [32768], P(('grow', 'gcol')), may hold values from 0.1 to 10
- mixing: float32 [1024, 1024], P('grow', 'gcol'), may hold values from -0.1875 to 0.1875
Outputs:
- residual: float32 [32768, 1024], P(('grow', 'gcol'))
- projected: float32 [1024, 1024], P('grow', 'gcol')
The draws below stay inside these ranges and needn't reach their ends.
All inputs are finite; a program needn't handle non-finite values.
Results may differ from the reference program's by a relative error of at most 0.000073.
Values sent between devices are 32-bit elements; how exact they have to be, the bound alone decides.
No kernel may reach another device: no remote copies, remote signals or barrier semaphores. Data moves between devices by JAX's collectives and lax.ppermute only.
A program may use at most 128 MiB of HBM per device.

```python
import math
import jax
import jax.numpy as jnp
from jax import lax

NB = 1024
ROWS = 32768


def spiked(result, rng, source, target, blocks, factor):
    owner, partner = [(jnp.arange(result.shape[position]) // (result.shape[position] // blocks)).reshape([-1 if axis == position else 1 for axis in range(result.ndim)]) for position in (source, target)]
    chosen = jax.random.permutation(rng, blocks)[partner]
    strong = (owner == chosen) | (owner == (partner + blocks // 2) % blocks)
    return jnp.where(strong, factor * result, result)


def steps_of(stream_key, shape, split, least, high):
    factor_of = 1.0
    for position, blocks in split:
        steps = jax.random.uniform(jax.random.fold_in(jax.random.fold_in(stream_key, 6), position), (blocks,), jnp.float32, least / len(split), high / len(split))
        factor_of = factor_of * jnp.repeat(jnp.exp(steps), shape[position] // blocks).reshape((-1,) + (1,) * (len(shape) - 1 - position))
    return factor_of


def normal_values(key, shape, spread, reach, shards=(), dtype=jnp.bfloat16):
    values = jax.random.normal(key, shape, jnp.float32) * spread
    if len(shards) > 0:
        values = steps_of(key, shape, shards, -0.22, 0.18) * values
    return jnp.clip(values, min=-reach, max=reach).astype(dtype)


def heavy_noise(own_key, dims, spread, reach, shards, heavy, held_as=jnp.bfloat16):
    values = spread * jax.random.normal(own_key, dims, jnp.float32)
    if shards:
        values = values * steps_of(own_key, dims, shards, -0.22, 0.18)
    return jnp.clip(spiked(values, jax.random.fold_in(own_key, 3), *heavy), -reach, reach).astype(held_as)


def setup_inputs(seed: int = 0) -> dict:
    keys = jax.random.split(jax.random.key(seed), 5)
    psi = normal_values(keys[0], (ROWS, NB), 1.0, 6.0, ((0, 32),), jnp.float32)
    vpsi = heavy_noise(keys[1], (ROWS, NB), 1.0, 6.0, ((0, 32),), (0, 1, 32, 2.75), jnp.float32)
    kinetic = jnp.clip(jnp.exp(math.log(10.0) - 4.6051702 * jax.random.uniform(keys[2], (ROWS,), jnp.float32) ** steps_of(keys[2], (ROWS,), ((0, 32),), -0.2, 0.2)), 0.1, 10.0)
    mixing = normal_values(keys[3], (NB, NB), NB ** -0.5, 0.1875, ((0, 4), (1, 8)), jnp.float32)
    return dict(psi=psi, vpsi=vpsi, kinetic=kinetic, mixing=mixing)


def reference(psi, vpsi, kinetic, mixing):
    hpsi = kinetic[:, None] * psi + vpsi
    projected = lax.dot_general(psi, hpsi, (((0,), (0,)), ((), ())), precision=lax.Precision.HIGHEST, preferred_element_type=jnp.float32) * (1.0 / ROWS)
    correction = hpsi - jnp.dot(psi, projected, precision=lax.Precision.HIGHEST, preferred_element_type=jnp.float32)
    residual = jnp.dot(correction, mixing, precision=lax.Precision.HIGHEST, preferred_element_type=jnp.float32)
    return residual, projected
```

```python
import functools

import jax
import jax.numpy as jnp
from jax import lax
from jax.experimental import pallas as pl
from jax.experimental.pallas import tpu as pltpu
from jax.sharding import PartitionSpec as P


F32, BF16 = jnp.float32, jnp.bfloat16
CHAINS = 2


def split(x):
    high = x.astype(BF16)
    return high, (x - high.astype(F32)).astype(BF16)


def mm(a, b, dims=((1,), (0,))):
    return lax.dot_general(a, b, (dims, ((), ())), preferred_element_type=F32)


def mm3(a, b):
    (ah, al), (bh, bl) = a, b
    return mm(ah, bh) + (mm(al, bh) + mm(ah, bl))


def cost(flops, nbytes):
    return pl.CostEstimate(flops=flops, bytes_accessed=nbytes, transcendentals=0)


def params(mib):
    return pltpu.CompilerParams(dimension_semantics=("arbitrary",), vmem_limit_bytes=mib << 20)


def column(x):
    n, lanes = x.shape
    eye = lax.broadcasted_iota(jnp.int32, (lanes, lanes), 0) == lax.broadcasted_iota(jnp.int32, (lanes, lanes), 1)
    return jnp.concatenate([jnp.sum(jnp.where(eye, x[i : i + 1], 0.0), 1, keepdims=True) for i in range(n)], 0)


def share_kernel(dims, scale, core_ref, psi_ref, vpsi_ref, kin_ref, *rest):
    G, Z, b, bc = dims
    outs, (ph_ref, pl_ref, hh_ref, hl_ref, acc) = rest[: 2 * CHAINS], rest[2 * CHAINS :]
    r = pl.program_id(0)
    psi = psi_ref[...]
    h = column(kin_ref[0]) * psi + vpsi_ref[...]
    ph, pl_ = split(psi)
    hh, hl = split(h)
    hh_ref[...], hl_ref[...] = hh, hl
    for k in range(CHAINS):
        for g in range(G):
            to, at = slice(g * b, (g + 1) * b), slice((g * CHAINS + k) * b, (g * CHAINS + k + 1) * b)
            ph_ref[k, :, to], pl_ref[k, :, to] = ph[:, at], pl_[:, at]
    pht = ph.T
    left = jnp.concatenate([pht, pl_.T, pht], 1)
    right = jnp.concatenate([hh, hh, hl], 0)
    n = psi.shape[1]
    t = 256

    @pl.when(r == 0)
    def _():
        for j in range(n // t):
            acc[:, j * t : (j + 1) * t] = mm(left, right[:, j * t : (j + 1) * t])

    @pl.when(r > 0)
    def _():
        for j in range(n // t):
            acc[:, j * t : (j + 1) * t] += mm(left, right[:, j * t : (j + 1) * t])

    @pl.when(r == pl.num_programs(0) - 1)
    def _():
        core = core_ref[0]
        half = n // 2
        br = n // G
        for side, c in enumerate((core, 1 - core)):
            cols = pl.ds(pl.multiple_of(c * half, half), half)
            for k in range(CHAINS):
                out = outs[2 * k + side]
                for g in range(G):
                    x = acc[g * br + k * b : g * br + (k + 1) * b, cols] * scale
                    for z in range(Z):
                        out[g, z] = x[:, z * bc : (z + 1) * bc]


def share(core, psi, vpsi, kin, dims, scale):
    G, _, b, _ = dims
    rows, bands = psi.shape
    t = 256
    blk = pl.BlockSpec((t, bands), lambda i, c: (i, 0))
    whole = pl.BlockSpec(dims, lambda i, c: (0, 0, 0, 0))
    chain = pl.BlockSpec((CHAINS, t, G * b), lambda i, c: (0, i, 0))
    return pl.pallas_call(
        functools.partial(share_kernel, dims, scale),
        grid_spec=pltpu.PrefetchScalarGridSpec(
            num_scalar_prefetch=1,
            grid=(rows // t,),
            in_specs=[blk, blk, pl.BlockSpec((1, t // 128, 128), lambda i, c: (i, 0, 0))],
            out_specs=[whole] * (2 * CHAINS) + [chain] * 2 + [blk] * 2,
            scratch_shapes=[pltpu.VMEM((bands, bands), F32)],
        ),
        out_shape=[jax.ShapeDtypeStruct(dims, F32)] * (2 * CHAINS)
        + [pltpu.HBM((CHAINS, rows, G * b), BF16)] * 2
        + [pltpu.HBM((rows, bands), BF16)] * 2,
        compiler_params=params(26),
        cost_estimate=cost(6 * rows * bands * bands, 12 * rows * bands),
        name="share",
    )(core, *(pltpu.with_memory_space_constraint(x, pltpu.HBM) for x in (psi, vpsi)), kin.reshape(rows // t, t // 128, 128))


def joined_kernel(core_ref, own_ref, sib_ref, high_ref, low_ref):
    G, Z, br, bc = own_ref.shape
    core = core_ref[0]
    for c, ref in ((core, own_ref), (1 - core, sib_ref)):
        for g in range(G):
            for z in range(Z):
                at = slice(g * br, (g + 1) * br), pl.ds(pl.multiple_of((2 * z + c) * bc, bc), bc)
                high_ref[at], low_ref[at] = split(ref[g, z])


def joined(core, own, sib):
    G, _, br, bc = own.shape
    bands = G * br
    if bc % 128:
        return split(ordered(own, sib, core[0], 2).transpose(0, 3, 1, 2, 4).reshape(bands, bands))
    whole = pl.BlockSpec(own.shape, lambda i, c: (0, 0, 0, 0))
    return pl.pallas_call(
        joined_kernel,
        grid_spec=pltpu.PrefetchScalarGridSpec(
            num_scalar_prefetch=1,
            grid=(1,),
            in_specs=[whole, whole],
            out_specs=[pl.BlockSpec((bands, bands), lambda i, c: (0, 0))] * 2,
        ),
        out_shape=[jax.ShapeDtypeStruct((bands, bands), BF16)] * 2,
        compiler_params=params(14),
        cost_estimate=cost(100 * bands * bands, 12 * bands * bands),
        name="joined",
    )(core, own, sib)


def mixed_kernel(hh_ref, hl_ref, mh_ref, ml_ref, out_ref):
    n = mh_ref.shape[1]
    for j in range(n // 512):
        s = slice(j * 512, (j + 1) * 512)
        out_ref[:, s] = mm3((hh_ref[...], hl_ref[...]), (mh_ref[:, s], ml_ref[:, s]))


def mixed(h, m):
    rows, bands = h[0].shape
    t = 256
    blk = pl.BlockSpec((t, bands), lambda i: (i, 0))
    return pl.pallas_call(
        mixed_kernel,
        grid=(rows // t,),
        in_specs=[blk, blk] + [pl.BlockSpec((bands, bands), lambda i: (0, 0))] * 2,
        out_specs=blk,
        out_shape=jax.ShapeDtypeStruct((rows, bands), F32),
        compiler_params=params(14),
        cost_estimate=cost(6 * rows * bands * bands, 16 * rows * bands),
        name="mixed",
    )(*h, *m)


def turned_kernel(core_ref, own_ref, sib_ref, m1h, m1l, m2h, m2l, out_ref):
    out_ref[...] = mm3(split(own_ref[...]), (m1h[...], m1l[...])) + mm3(split(sib_ref[...]), (m2h[...], m2l[...]))


def turned(core, own, sib, m):
    b, half = own.shape
    row = pl.BlockSpec((b, half), lambda i, c: (0, 0))
    m1 = pl.BlockSpec((half, half), lambda i, c: (c[0], c[0]))
    m2 = pl.BlockSpec((half, half), lambda i, c: (1 - c[0], c[0]))
    return pl.pallas_call(
        turned_kernel,
        grid_spec=pltpu.PrefetchScalarGridSpec(
            num_scalar_prefetch=1, grid=(1,), in_specs=[row, row, m1, m1, m2, m2], out_specs=row
        ),
        out_shape=jax.ShapeDtypeStruct((b, half), F32),
        compiler_params=params(8),
        cost_estimate=cost(12 * b * half * half, 8 * half * half),
        name="turned",
    )(core, own, sib, *m, *m)


def less_kernel(core_ref, acc_ref, ph_ref, pl_ref, own_ref, sib_ref, out_ref, wh, wl):
    n = own_ref.shape[1]
    core = core_ref[0]

    @pl.when(pl.program_id(0) == 0)
    def _():
        wh[0], wl[0] = split(own_ref[...])
        wh[1], wl[1] = split(sib_ref[...])

    for j in range(2):
        s = pl.ds(pl.multiple_of(jnp.where(core == j, 0, 1) * n, n), n)
        out_ref[:, s] = acc_ref[:, s] - mm3((ph_ref[...], pl_ref[...]), (wh[j], wl[j]))


def less(core, acc, psi, own, sib, k):
    rows, bands = acc.shape
    kk, half = own.shape
    t = 256
    blk = pl.BlockSpec((t, bands), lambda i, c: (i, 0))
    part = pl.BlockSpec((None, t, kk), lambda i, c: (k, i, 0))
    w = pl.BlockSpec((kk, half), lambda i, c: (0, 0))
    return pl.pallas_call(
        less_kernel,
        grid_spec=pltpu.PrefetchScalarGridSpec(
            num_scalar_prefetch=1,
            grid=(rows // t,),
            in_specs=[blk, part, part, w, w],
            out_specs=blk,
            scratch_shapes=[pltpu.VMEM((2, kk, half), BF16)] * 2,
        ),
        out_shape=jax.ShapeDtypeStruct((rows, bands), F32),
        compiler_params=params(14),
        cost_estimate=cost(6 * rows * kk * bands, 16 * rows * bands),
        name="less",
    )(core, acc, *psi, own, sib)


def pick(x, i, axis):
    return lax.dynamic_index_in_dim(x, i, axis, keepdims=False)


def hop(x, axis, mask):
    n = lax.axis_size(axis)
    return lax.ppermute(x, axis, [(i, i ^ mask) for i in range(n)])


def bit_of(axis, mask):
    return jnp.where((lax.axis_index(axis) & mask) != 0, 1, 0)


def ordered(mine, theirs, bit, axis):
    low = bit == 0
    return jnp.stack([jnp.where(low, mine, theirs), jnp.where(low, theirs, mine)], axis)


def scatter(x, bits, order):
    bits = list(bits)
    for bit in order:
        a = bits.index(bit)
        mine = bit_of(*bit)
        x = pick(x, mine, a) + hop(pick(x, 1 - mine, a), *bit)
        bits.remove(bit)
    return x


def gather(x, bits, order, have=()):
    have = list(have)
    for bit in order:
        a = sum(bits.index(other) < bits.index(bit) for other in have)
        x = ordered(x, hop(x, *bit), bit_of(*bit), a)
        have.append(bit)
    return x


def after(x, *others):
    return lax.optimization_barrier((x, *others))[0]


def axis_bits(axis, low):
    n = lax.axis_size(axis)
    return [(axis, 1 << i) for i in range(low, n.bit_length() - 1)][::-1]


def body(psi, vpsi, kinetic, mixing):
    G, C = lax.axis_size("grow"), lax.axis_size("gcol")
    rows, bands = psi.shape
    Z = C // 2
    br, bc, half = bands // G, bands // C, bands // 2
    b = br // CHAINS
    gb, zb = axis_bits("grow", 0), axis_bits("gcol", 1)
    up = gb[::-1]
    core = lax.axis_index("gcol") % 2
    core1 = core.reshape(1)

    *pieces, ph, pl_, hh, hl = share(core1, psi, vpsi, kinetic, (G, Z, b, bc), 1.0 / (rows * G * C))

    m = gather(after(mixing, pieces[0]), zb, zb)
    ma = gather(m[..., : br // 2, :], gb, up).reshape(G, Z, br // 2, bc)
    mb = gather(m[..., br // 2 :, :], gb, gb).reshape(G, Z, br // 2, bc)
    m_own = jnp.concatenate([ma, mb], 2)
    m_all = joined(core1, m_own, hop(m_own, "gcol", 1))
    acc = mixed((hh, hl), m_all)

    h_parts = []
    for k in range(CHAINS):
        there, back = (up, gb) if k % 2 == 0 else (gb, up)
        q = pieces[2 * k] + hop(pieces[2 * k + 1], "gcol", 1)
        q = q.reshape((2,) * (len(gb) + len(zb)) + (b, bc))
        q = scatter(q, gb + zb, there + zb[:0:-1])
        q = q + hop(q, *zb[0])
        h_parts.append(pick(q, bit_of(*zb[0]), 0))
        row = gather(q, zb, zb[1:], zb[:1]).reshape(Z, b, bc).transpose(1, 0, 2).reshape(b, half)
        w = turned(core1, row, hop(row, "gcol", 1), m_all)
        w = gather(w, gb, back).reshape(G * b, half)
        acc = less(core1, acc, (ph, pl_), w, hop(w, "gcol", 1), k)

    h = jnp.concatenate(h_parts, 0)
    projected = lax.ppermute(h, "gcol", [(i, (i % 2) * Z + i // 2) for i in range(C)])
    return acc, projected


def solution(mesh):
    return jax.shard_map(
        body,
        mesh=mesh,
        in_specs=(
            P(("grow", "gcol"), None),
            P(("grow", "gcol"), None),
            P(("grow", "gcol")),
            P("grow", "gcol"),
        ),
        out_specs=(P(("grow", "gcol"), None), P("grow", "gcol")),
        check_vma=False,
    )
```

```python
import functools

import jax
import jax.numpy as jnp
from jax import lax
from jax.experimental import pallas as pl
from jax.experimental.pallas import tpu as pltpu
from jax.sharding import PartitionSpec as P


F32, BF16 = jnp.float32, jnp.bfloat16
CHAINS = 2


def split(x):
    high = x.astype(BF16)
    return high, (x - high.astype(F32)).astype(BF16)


def mm(a, b, dims=((1,), (0,))):
    return lax.dot_general(a, b, (dims, ((), ())), preferred_element_type=F32)


def mm3(a, b):
    (ah, al), (bh, bl) = a, b
    return mm(ah, bh) + (mm(al, bh) + mm(ah, bl))


def cost(flops, nbytes):
    return pl.CostEstimate(flops=flops, bytes_accessed=nbytes, transcendentals=0)


def params(mib):
    return pltpu.CompilerParams(dimension_semantics=("arbitrary",), vmem_limit_bytes=mib << 20)


def column(x):
    n, lanes = x.shape
    eye = lax.broadcasted_iota(jnp.int32, (lanes, lanes), 0) == lax.broadcasted_iota(jnp.int32, (lanes, lanes), 1)
    return jnp.concatenate([jnp.sum(jnp.where(eye, x[i : i + 1], 0.0), 1, keepdims=True) for i in range(n)], 0)


def pieces_of(x, out, dims):
    G, Z, b, bc = dims
    for g in range(G):
        for z in range(Z):
            out[g, z] = x[g * b : (g + 1) * b, z * bc : (z + 1) * bc]


def first_kernel(dims, core_ref, psi_ref, vpsi_ref, kin_ref, *rest):
    G, _, b, _ = dims
    outs, (ph_ref, pl_ref, hh_ref, hl_ref, th_ref, tl_ref, acc, right) = rest[:CHAINS], rest[CHAINS:]
    r = pl.program_id(0)
    psi = psi_ref[...]
    h = column(kin_ref[0]) * psi + vpsi_ref[...]
    ph, pl_ = split(psi)
    hh, hl = split(h)
    _, n = psi.shape
    half = n // 2
    hh_ref[...], hl_ref[...] = hh, hl
    rows = [slice((g * CHAINS + k) * b, (g * CHAINS + k + 1) * b) for k in range(CHAINS) for g in range(G)]
    for k in range(CHAINS):
        ph_ref[k] = jnp.concatenate([ph[:, at] for at in rows[k * G : (k + 1) * G]], 1)
        pl_ref[k] = jnp.concatenate([pl_[:, at] for at in rows[k * G : (k + 1) * G]], 1)
    th = jnp.concatenate([ph[:, at] for at in rows], 1).T
    tl = jnp.concatenate([pl_[:, at] for at in rows], 1).T
    th_ref[...], tl_ref[...] = th, tl
    left = jnp.concatenate([th, tl, th], 1)
    right[...] = jnp.concatenate([hh, hh, hl], 0)
    w = 256
    sib = (1 - core_ref[0]) * half

    @pl.when(r == 0)
    def _():
        acc[...] = jnp.zeros_like(acc)

    for j in range(0, half, w):
        acc[:, j : j + w] += mm(left, right[:, pl.ds(pl.multiple_of(sib + j, w), w)])

    @pl.when(r == pl.num_programs(0) - 1)
    def _():
        for k in range(CHAINS):
            pieces_of(acc[k * G * b : (k + 1) * G * b, :], outs[k], dims)


def first(core, psi, vpsi, kin, dims):
    G, _, b, _ = dims
    rows, bands = psi.shape
    t = 256
    blk = pl.BlockSpec((t, bands), lambda i, c: (i, 0))
    piece = pl.BlockSpec(dims, lambda i, c: (0, 0, 0, 0))
    chain = pl.BlockSpec((CHAINS, t, G * b), lambda i, c: (0, i, 0))
    turn = pl.BlockSpec((bands, t), lambda i, c: (0, i))
    return pl.pallas_call(
        functools.partial(first_kernel, dims),
        grid_spec=pltpu.PrefetchScalarGridSpec(
            num_scalar_prefetch=1,
            grid=(rows // t,),
            in_specs=[blk, blk, pl.BlockSpec((1, t // 128, 128), lambda i, c: (i, 0, 0))],
            out_specs=[piece] * CHAINS + [chain] * 2 + [blk] * 2 + [turn] * 2,
            scratch_shapes=[pltpu.VMEM((bands, bands // 2), F32), pltpu.VMEM((3 * t, bands), BF16)],
        ),
        out_shape=[jax.ShapeDtypeStruct(dims, F32)] * CHAINS
        + [pltpu.HBM((CHAINS, rows, G * b), BF16)] * 2
        + [jax.ShapeDtypeStruct((rows, bands), BF16)] * 2
        + [jax.ShapeDtypeStruct((bands, rows), BF16)] * 2,
        compiler_params=params(20),
        cost_estimate=cost(3 * rows * bands * bands, 12 * rows * bands),
        name="first",
    )(core, *(pltpu.with_memory_space_constraint(x, pltpu.HBM) for x in (psi, vpsi)), kin.reshape(rows // t, t // 128, 128))


def second_kernel(dims, core_ref, th_ref, tl_ref, hh_ref, hl_ref, *outs):
    left = jnp.concatenate([th_ref[...], tl_ref[...], th_ref[...]], 1)
    right = jnp.concatenate([hh_ref[...], hh_ref[...], hl_ref[...]], 0)
    pieces_of(mm(left, right), outs[0], dims)


def second(core, turned_psi, h, dims, k):
    G, _, b, _ = dims
    bands, rows = turned_psi[0].shape
    left = pl.BlockSpec((G * b, rows), lambda i, c: (k, 0))
    right = pl.BlockSpec((rows, bands // 2), lambda i, c: (0, c[0]))
    return pl.pallas_call(
        functools.partial(second_kernel, dims),
        grid_spec=pltpu.PrefetchScalarGridSpec(
            num_scalar_prefetch=1,
            grid=(1,),
            in_specs=[left, left, right, right],
            out_specs=pl.BlockSpec(dims, lambda i, c: (0, 0, 0, 0)),
        ),
        out_shape=jax.ShapeDtypeStruct(dims, F32),
        compiler_params=params(6),
        cost_estimate=cost(3 * rows * G * b * bands, 4 * rows * bands),
        name="second",
    )(core, *turned_psi, *h)


def joined_kernel(core_ref, own_ref, sib_ref, high_ref, low_ref):
    G, Z, br, bc = own_ref.shape
    core = core_ref[0]
    for c, ref in ((core, own_ref), (1 - core, sib_ref)):
        for g in range(G):
            for z in range(Z):
                at = slice(g * br, (g + 1) * br), pl.ds(pl.multiple_of((2 * z + c) * bc, bc), bc)
                high_ref[at], low_ref[at] = split(ref[g, z])


def joined(core, own, sib):
    G, _, br, bc = own.shape
    bands = G * br
    if bc % 128:
        return split(ordered(own, sib, core[0] == 1, 2).transpose(0, 3, 1, 2, 4).reshape(bands, bands))
    whole = pl.BlockSpec(own.shape, lambda i, c: (0, 0, 0, 0))
    return pl.pallas_call(
        joined_kernel,
        grid_spec=pltpu.PrefetchScalarGridSpec(
            num_scalar_prefetch=1,
            grid=(1,),
            in_specs=[whole, whole],
            out_specs=[pl.BlockSpec((bands, bands), lambda i, c: (0, 0))] * 2,
        ),
        out_shape=[jax.ShapeDtypeStruct((bands, bands), BF16)] * 2,
        compiler_params=params(6),
        cost_estimate=cost(100 * bands * bands, 12 * bands * bands),
        name="joined",
    )(core, own, sib)


def mixed_kernel(hh_ref, hl_ref, mh_ref, ml_ref, out_ref):
    n = mh_ref.shape[1]
    for j in range(n // 512):
        s = slice(j * 512, (j + 1) * 512)
        out_ref[:, s] = mm3((hh_ref[...], hl_ref[...]), (mh_ref[:, s], ml_ref[:, s]))


def mixed(h, m):
    rows, bands = h[0].shape
    t = 512
    blk = pl.BlockSpec((t, bands), lambda i: (i, 0))
    return pl.pallas_call(
        mixed_kernel,
        grid=(rows // t,),
        in_specs=[blk, blk] + [pl.BlockSpec((bands, bands), lambda i: (0, 0))] * 2,
        out_specs=blk,
        out_shape=jax.ShapeDtypeStruct((rows, bands), F32),
        compiler_params=params(20),
        cost_estimate=cost(6 * rows * bands * bands, 16 * rows * bands),
        name="mixed",
    )(*h, *m)


def turned_kernel(core_ref, own_ref, sib_ref, m1h, m1l, m2h, m2l, out_ref):
    out_ref[...] = mm3(split(own_ref[...]), (m1h[...], m1l[...])) + mm3(split(sib_ref[...]), (m2h[...], m2l[...]))


def turned(core, own, sib, m):
    b, half = own.shape
    row = pl.BlockSpec((b, half), lambda i, c: (0, 0))
    m1 = pl.BlockSpec((half, half), lambda i, c: (c[0], c[0]))
    m2 = pl.BlockSpec((half, half), lambda i, c: (1 - c[0], c[0]))
    return pl.pallas_call(
        turned_kernel,
        grid_spec=pltpu.PrefetchScalarGridSpec(
            num_scalar_prefetch=1, grid=(1,), in_specs=[row, row, m1, m1, m2, m2], out_specs=row
        ),
        out_shape=jax.ShapeDtypeStruct((b, half), F32),
        compiler_params=params(5),
        cost_estimate=cost(12 * b * half * half, 8 * half * half),
        name="turned",
    )(core, own, sib, *m, *m)


def less_kernel(core_ref, acc_ref, ph_ref, pl_ref, *rest):
    ws, (out_ref, right) = rest[:CHAINS], rest[-2:]
    kk = CHAINS * ws[0].shape[0]

    @pl.when(pl.program_id(0) == 0)
    def _():
        high, low = split(jnp.concatenate([w[...] for w in ws], 0))
        right[:kk], right[kk : 2 * kk], right[2 * kk :] = high, high, low

    high, low = [ph_ref[k] for k in range(CHAINS)], [pl_ref[k] for k in range(CHAINS)]
    out_ref[...] = acc_ref[...] - mm(jnp.concatenate(high + low + high, 1), right[...])


def less(core, acc, psi, ws, into=None):
    other = into is not None
    rows, bands = acc.shape
    kk, half = ws[0].shape
    t = 512
    blk = pl.BlockSpec((t, half), lambda i, c: (i, 1 - c[0] if other else c[0]))
    part = pl.BlockSpec((CHAINS, t, kk), lambda i, c: (0, i, 0))
    w = pl.BlockSpec((kk, half), lambda i, c: (0, 0))
    return pl.pallas_call(
        less_kernel,
        grid_spec=pltpu.PrefetchScalarGridSpec(
            num_scalar_prefetch=1,
            grid=(rows // t,),
            in_specs=[blk, part, part] + [w] * CHAINS + [pl.BlockSpec(memory_space=pl.ANY)] * other,
            out_specs=blk,
            scratch_shapes=[pltpu.VMEM((3 * CHAINS * kk, half), BF16)],
        ),
        out_shape=pltpu.HBM((rows, bands), F32),
        input_output_aliases={4 + CHAINS: 0} if other else {},
        compiler_params=params(24),
        cost_estimate=cost(3 * rows * kk * CHAINS * bands, 8 * rows * bands),
        name="less",
    )(core, acc, *psi, *ws, *([into] if other else []))


def halves(x, one, axis):
    low, high = (lax.index_in_dim(x, i, axis, keepdims=False) for i in (0, 1))
    return jnp.where(one, high, low), jnp.where(one, low, high)


def hop(x, axis, mask):
    n = lax.axis_size(axis)
    return lax.ppermute(x, axis, [(i, i ^ mask) for i in range(n)])


def ordered(mine, theirs, one, axis):
    return jnp.stack([jnp.where(one, theirs, mine), jnp.where(one, mine, theirs)], axis)


def reduced(x, place, bits, bit):
    keep, give = halves(x, place[bit], bits.index(bit))
    return keep + hop(give, *bit)


def gather(x, place, bits, order, have=()):
    have = list(have)
    for bit in order:
        a = sum(bits.index(other) < bits.index(bit) for other in have)
        got = hop(x, *bit)
        x = ordered(x, got, place[bit], a)
        have.append(bit)
    return x


def after(x, *others):
    if not others:
        return x
    return lax.optimization_barrier((x, *others))[0]


def axis_bits(axis, low):
    n = lax.axis_size(axis)
    return [(axis, 1 << i) for i in range(low, n.bit_length() - 1)][::-1]


def body(psi, vpsi, kinetic, mixing):
    G, C = lax.axis_size("grow"), lax.axis_size("gcol")
    rows, bands = psi.shape
    Z = C // 2
    br, bc, half = bands // G, bands // C, bands // 2
    b = br // CHAINS
    gb, zb = axis_bits("grow", 0), axis_bits("gcol", 1)
    up = gb[::-1]
    place = {bit: (lax.axis_index(bit[0]) & bit[1]) != 0 for bit in gb + zb}
    core1 = (lax.axis_index("gcol") % 2).reshape(1)
    psi, core1, place = lax.optimization_barrier((psi, core1, place))

    dims = (G, Z, b, bc)
    scale = 1.0 / (rows * G * C)
    *theirs, ph, pl_, hh, hl, th, tl = first(core1, psi, vpsi, kinetic, dims)
    ours = [second(core1, (th, tl), (hh, hl), dims, k) for k in range(CHAINS)]

    sums = []
    for k in range(CHAINS):
        q = ours[k] + hop(theirs[k], "gcol", 1)
        sums.append(q.reshape((2,) * (len(gb) + len(zb)) + (b, bc)))
    left = [gb + zb for _ in range(CHAINS)]
    route = [(up if k % 2 == 0 else gb) + zb[:0:-1] for k in range(CHAINS)]
    for i in range(len(route[0])):
        for k in range(CHAINS):
            bit = route[k][i]
            sums[k] = reduced(sums[k], place, left[k], bit)
            left[k] = [other for other in left[k] if other != bit]
    sums = [(q + hop(q, *zb[0])) * scale for q in sums]

    m = gather(after(mixing, theirs[0]), place, zb, zb)
    ma = gather(m[..., : br // 2, :], place, gb, up).reshape(G, Z, br // 2, bc)
    mb = gather(m[..., br // 2 :, :], place, gb, gb).reshape(G, Z, br // 2, bc)
    m_own = jnp.concatenate([ma, mb], 2)
    m_all = joined(core1, m_own, hop(m_own, "gcol", 1))
    acc = mixed((hh, hl), m_all)

    h_parts, w_own, w_sib = [], [], []
    for k, q in enumerate(sums):
        back = gb if k % 2 == 0 else up
        h_parts.append(halves(q, place[zb[0]], 0)[0])
        row = gather(q, place, zb, zb[1:], zb[:1]).reshape(Z, b, bc).transpose(1, 0, 2).reshape(b, half)
        w = turned(core1, row, hop(row, "gcol", 1), m_all)
        w = gather(w, place, gb, back).reshape(G * b, half)
        w_own.append(w)
        w_sib.append(hop(w, "gcol", 1))

    h = jnp.concatenate(h_parts, 0)
    projected = lax.ppermute(h, "gcol", [(i, (i % 2) * Z + i // 2) for i in range(C)])
    near = less(core1, acc, (ph, pl_), w_own)
    return less(core1, acc, (ph, pl_), w_sib, near), projected


def solution(mesh):
    return jax.shard_map(
        body,
        mesh=mesh,
        in_specs=(
            P(("grow", "gcol"), None),
            P(("grow", "gcol"), None),
            P(("grow", "gcol")),
            P("grow", "gcol"),
        ),
        out_specs=(P(("grow", "gcol"), None), P("grow", "gcol")),
        check_vma=False,
    )
```

```python
import functools

import jax
import jax.numpy as jnp
from jax import lax
from jax.experimental import pallas as pl
from jax.experimental.pallas import tpu as pltpu
from jax.sharding import PartitionSpec as P


F32, BF16 = jnp.float32, jnp.bfloat16
CHAINS = 2


def split(x):
    high = x.astype(BF16)
    return high, (x - high.astype(F32)).astype(BF16)


def mm(a, b, dims=((1,), (0,))):
    return lax.dot_general(a, b, (dims, ((), ())), preferred_element_type=F32)


def mm3(a, b):
    (ah, al), (bh, bl) = a, b
    return mm(ah, bh) + (mm(al, bh) + mm(ah, bl))


def cost(flops, nbytes):
    return pl.CostEstimate(flops=flops, bytes_accessed=nbytes, transcendentals=0)


def params(mib):
    return pltpu.CompilerParams(dimension_semantics=("arbitrary",), vmem_limit_bytes=mib << 20)


def column(x):
    n, lanes = x.shape
    eye = lax.broadcasted_iota(jnp.int32, (lanes, lanes), 0) == lax.broadcasted_iota(jnp.int32, (lanes, lanes), 1)
    return jnp.concatenate([jnp.sum(jnp.where(eye, x[i : i + 1], 0.0), 1, keepdims=True) for i in range(n)], 0)


def pieces_of(x, out, dims):
    G, Z, b, bc = dims
    for g in range(G):
        for z in range(Z):
            out[g, z] = x[g * b : (g + 1) * b, z * bc : (z + 1) * bc]


def first_kernel(dims, masks, core_ref, psi_ref, vpsi_ref, kin_ref, *rest):
    G, _, b, _ = dims
    outs, (ph_ref, pl_ref, hh_ref, hl_ref, th_ref, tl_ref, acc, right) = rest[:CHAINS], rest[CHAINS:]
    r = pl.program_id(0)
    psi = psi_ref[...]
    h = column(kin_ref[0]) * psi + vpsi_ref[...]
    ph, pl_ = split(psi)
    hh, hl = split(h)
    _, n = psi.shape
    half = n // 2
    hh_ref[...], hl_ref[...] = hh, hl
    rows = [slice((g * CHAINS + k) * b, (g * CHAINS + k + 1) * b) for k in range(CHAINS) for g in range(G)]
    for k in range(CHAINS):
        for v in range(2):
            some = [rows[k * G + g] for g in range(G) if (g & masks[k] != 0) == v]
            ph_ref[k, v] = jnp.concatenate([ph[:, at] for at in some], 1)
            pl_ref[k, v] = jnp.concatenate([pl_[:, at] for at in some], 1)
    th = jnp.concatenate([ph[:, at] for at in rows], 1).T
    tl = jnp.concatenate([pl_[:, at] for at in rows], 1).T
    th_ref[...], tl_ref[...] = th, tl
    left = jnp.concatenate([th, tl, th], 1)
    right[...] = jnp.concatenate([hh, hh, hl], 0)
    w = 256
    sib = (1 - core_ref[0]) * half

    @pl.when(r == 0)
    def _():
        acc[...] = jnp.zeros_like(acc)

    for j in range(0, half, w):
        acc[:, j : j + w] += mm(left, right[:, pl.ds(pl.multiple_of(sib + j, w), w)])

    @pl.when(r == pl.num_programs(0) - 1)
    def _():
        for k in range(CHAINS):
            pieces_of(acc[k * G * b : (k + 1) * G * b, :], outs[k], dims)


def first(core, psi, vpsi, kin, dims, masks):
    G, _, b, _ = dims
    rows, bands = psi.shape
    t = 256
    blk = pl.BlockSpec((t, bands), lambda i, c: (i, 0))
    piece = pl.BlockSpec(dims, lambda i, c: (0, 0, 0, 0))
    chain = pl.BlockSpec((CHAINS, 2, t, G * b // 2), lambda i, c: (0, 0, i, 0))
    turn = pl.BlockSpec((bands, t), lambda i, c: (0, i))
    return pl.pallas_call(
        functools.partial(first_kernel, dims, masks),
        grid_spec=pltpu.PrefetchScalarGridSpec(
            num_scalar_prefetch=1,
            grid=(rows // t,),
            in_specs=[blk, blk, pl.BlockSpec((1, t // 128, 128), lambda i, c: (i, 0, 0))],
            out_specs=[piece] * CHAINS + [chain] * 2 + [blk] * 2 + [turn] * 2,
            scratch_shapes=[pltpu.VMEM((bands, bands // 2), F32), pltpu.VMEM((3 * t, bands), BF16)],
        ),
        out_shape=[jax.ShapeDtypeStruct(dims, F32)] * CHAINS
        + [pltpu.HBM((CHAINS, 2, rows, G * b // 2), BF16)] * 2
        + [jax.ShapeDtypeStruct((rows, bands), BF16)] * 2
        + [jax.ShapeDtypeStruct((bands, rows), BF16)] * 2,
        compiler_params=params(20),
        cost_estimate=cost(3 * rows * bands * bands, 12 * rows * bands),
        name="first",
    )(core, *(pltpu.with_memory_space_constraint(x, pltpu.HBM) for x in (psi, vpsi)), kin.reshape(rows // t, t // 128, 128))


def second_kernel(dims, core_ref, th_ref, tl_ref, hh_ref, hl_ref, *outs):
    left = jnp.concatenate([th_ref[...], tl_ref[...], th_ref[...]], 1)
    right = jnp.concatenate([hh_ref[...], hh_ref[...], hl_ref[...]], 0)
    pieces_of(mm(left, right), outs[0], dims)


def second(core, turned_psi, h, dims, k):
    G, _, b, _ = dims
    bands, rows = turned_psi[0].shape
    left = pl.BlockSpec((G * b, rows), lambda i, c: (k, 0))
    right = pl.BlockSpec((rows, bands // 2), lambda i, c: (0, c[0]))
    return pl.pallas_call(
        functools.partial(second_kernel, dims),
        grid_spec=pltpu.PrefetchScalarGridSpec(
            num_scalar_prefetch=1,
            grid=(1,),
            in_specs=[left, left, right, right],
            out_specs=pl.BlockSpec(dims, lambda i, c: (0, 0, 0, 0)),
        ),
        out_shape=jax.ShapeDtypeStruct(dims, F32),
        compiler_params=params(6),
        cost_estimate=cost(3 * rows * G * b * bands, 4 * rows * bands),
        name="second",
    )(core, *turned_psi, *h)


def joined_kernel(core_ref, *rest):
    refs, (high_ref, low_ref) = rest[:4], rest[4:]
    G, Z, n, bc = refs[0].shape
    core = core_ref[0]
    for i, ref in enumerate(refs):
        c, part = (core if i < 2 else 1 - core), i % 2
        for g in range(G):
            rows = slice((2 * g + part) * n, (2 * g + part + 1) * n)
            for z in range(Z):
                at = rows, pl.ds(pl.multiple_of((2 * z + c) * bc, bc), bc)
                high_ref[at], low_ref[at] = split(ref[g, z])


def joined(core, own, sib):
    G, Z, n, bc = own[0].shape
    bands = 2 * G * n
    if bc % 128:
        own, sib = (jnp.stack(x, 2).reshape(G, Z, 2 * n, bc) for x in (own, sib))
        return split(ordered(own, sib, core[0] == 1, 2).transpose(0, 3, 1, 2, 4).reshape(bands, bands))
    whole = pl.BlockSpec(own[0].shape, lambda i, c: (0, 0, 0, 0))
    return pl.pallas_call(
        joined_kernel,
        grid_spec=pltpu.PrefetchScalarGridSpec(
            num_scalar_prefetch=1,
            grid=(1,),
            in_specs=[whole] * 4,
            out_specs=[pl.BlockSpec((bands, bands), lambda i, c: (0, 0))] * 2,
        ),
        out_shape=[jax.ShapeDtypeStruct((bands, bands), BF16)] * 2,
        compiler_params=params(6),
        cost_estimate=cost(100 * bands * bands, 12 * bands * bands),
        name="joined",
    )(core, *own, *sib)


def mixed_kernel(hh_ref, hl_ref, mh_ref, ml_ref, out_ref):
    n = mh_ref.shape[1]
    for j in range(n // 512):
        s = slice(j * 512, (j + 1) * 512)
        out_ref[:, s] = mm3((hh_ref[...], hl_ref[...]), (mh_ref[:, s], ml_ref[:, s]))


def mixed(h, m):
    rows, bands = h[0].shape
    t = 512
    blk = pl.BlockSpec((t, bands), lambda i: (i, 0))
    return pl.pallas_call(
        mixed_kernel,
        grid=(rows // t,),
        in_specs=[blk, blk] + [pl.BlockSpec((bands, bands), lambda i: (0, 0))] * 2,
        out_specs=blk,
        out_shape=jax.ShapeDtypeStruct((rows, bands), F32),
        compiler_params=params(20),
        cost_estimate=cost(6 * rows * bands * bands, 16 * rows * bands),
        name="mixed",
    )(*h, *m)


def turned_kernel(core_ref, own_ref, sib_ref, m1h, m1l, m2h, m2l, out_ref):
    out_ref[...] = mm3(split(own_ref[...]), (m1h[...], m1l[...])) + mm3(split(sib_ref[...]), (m2h[...], m2l[...]))


def turned(core, own, sib, m):
    b, half = own.shape
    row = pl.BlockSpec((b, half), lambda i, c: (0, 0))
    m1 = pl.BlockSpec((half, half), lambda i, c: (c[0], c[0]))
    m2 = pl.BlockSpec((half, half), lambda i, c: (1 - c[0], c[0]))
    return pl.pallas_call(
        turned_kernel,
        grid_spec=pltpu.PrefetchScalarGridSpec(
            num_scalar_prefetch=1, grid=(1,), in_specs=[row, row, m1, m1, m2, m2], out_specs=row
        ),
        out_shape=jax.ShapeDtypeStruct((b, half), F32),
        compiler_params=params(5),
        cost_estimate=cost(12 * b * half * half, 8 * half * half),
        name="turned",
    )(core, own, sib, *m, *m)


def less_kernel(at_ref, acc_ref, *rest):
    high, low = [[x[...] for x in rest[k * CHAINS : (k + 1) * CHAINS]] for k in range(2)]
    ws, (out_ref, right) = rest[2 * CHAINS : 3 * CHAINS], rest[-2:]
    kk = CHAINS * ws[0].shape[0]

    @pl.when(pl.program_id(0) == 0)
    def _():
        wh, wl = split(jnp.concatenate([w[...] for w in ws], 0))
        right[:kk], right[kk : 2 * kk], right[2 * kk :] = wh, wh, wl

    out_ref[...] = acc_ref[...] - mm(jnp.concatenate(high + low + high, 1), right[...])


def less(at, acc, psi, ws, other_core, other_bands, into=None, last=False):
    rows, bands = acc.shape
    kk, half = ws[0].shape
    t = 512
    more = into is not None
    blk = pl.BlockSpec((t, half), lambda i, c: (i, 1 - c[0] if other_core else c[0]))

    def part(k):
        return pl.BlockSpec((None, None, t, kk), lambda i, c: (k, 1 - c[1 + k] if other_bands else c[1 + k], i, 0))

    w = pl.BlockSpec((kk, half), lambda i, c: (0, 0))
    shape = pltpu.HBM((rows, bands), F32) if last else jax.ShapeDtypeStruct((rows, bands), F32)
    return pl.pallas_call(
        less_kernel,
        grid_spec=pltpu.PrefetchScalarGridSpec(
            num_scalar_prefetch=1,
            grid=(rows // t,),
            in_specs=[blk]
            + [part(k) for k in range(CHAINS)] * 2
            + [w] * CHAINS
            + [pl.BlockSpec(memory_space=pl.ANY)] * more,
            out_specs=blk,
            scratch_shapes=[pltpu.VMEM((3 * CHAINS * kk, half), BF16)],
        ),
        out_shape=shape,
        input_output_aliases={2 + 3 * CHAINS: 0} if more else {},
        compiler_params=params(20),
        cost_estimate=cost(3 * rows * kk * CHAINS * bands, 8 * rows * bands),
        name="less",
    )(at, acc, *[x for x in psi for _ in range(CHAINS)], *ws, *([into] if more else []))


def halves(x, one, axis):
    low, high = (lax.index_in_dim(x, i, axis, keepdims=False) for i in (0, 1))
    return jnp.where(one, high, low), jnp.where(one, low, high)


def hop(x, axis, mask):
    n = lax.axis_size(axis)
    return lax.ppermute(x, axis, [(i, i ^ mask) for i in range(n)])


def ordered(mine, theirs, one, axis):
    return jnp.stack([jnp.where(one, theirs, mine), jnp.where(one, mine, theirs)], axis)


def reduced(x, place, bits, bit):
    keep, give = halves(x, place[bit], bits.index(bit))
    return keep + hop(give, *bit)


def gather(x, place, bits, order, have=()):
    have = list(have)
    for bit in order:
        a = sum(bits.index(other) < bits.index(bit) for other in have)
        got = hop(x, *bit)
        x = ordered(x, got, place[bit], a)
        have.append(bit)
    return x


def after(x, *others):
    if not others:
        return x
    return lax.optimization_barrier((x, *others))[0]


def axis_bits(axis, low):
    n = lax.axis_size(axis)
    return [(axis, 1 << i) for i in range(low, n.bit_length() - 1)][::-1]


def body(psi, vpsi, kinetic, mixing):
    G, C = lax.axis_size("grow"), lax.axis_size("gcol")
    rows, bands = psi.shape
    Z = C // 2
    br, bc, half = bands // G, bands // C, bands // 2
    b = br // CHAINS
    gb, zb = axis_bits("grow", 0), axis_bits("gcol", 1)
    up = gb[::-1]
    place = {bit: (lax.axis_index(bit[0]) & bit[1]) != 0 for bit in gb + zb}
    core1 = (lax.axis_index("gcol") % 2).reshape(1)
    backs = [gb if k % 2 == 0 else up for k in range(CHAINS)]
    at = jnp.concatenate([core1] + [place[back[-1]].astype(jnp.int32).reshape(1) for back in backs])
    psi, core1, at, place = lax.optimization_barrier((psi, core1, at, place))

    dims = (G, Z, b, bc)
    scale = 1.0 / (rows * G * C)
    *theirs, ph, pl_, hh, hl, th, tl = first(core1, psi, vpsi, kinetic, dims, [back[-1][1] for back in backs])
    ours = [second(core1, (th, tl), (hh, hl), dims, k) for k in range(CHAINS)]

    sums = []
    for k in range(CHAINS):
        q = ours[k] + hop(theirs[k], "gcol", 1)
        sums.append(q.reshape((2,) * (len(gb) + len(zb)) + (b, bc)))
    left = [gb + zb for _ in range(CHAINS)]
    route = [(up if k % 2 == 0 else gb) + zb[:0:-1] for k in range(CHAINS)]
    for i in range(len(route[0])):
        for k in range(CHAINS):
            bit = route[k][i]
            sums[k] = reduced(sums[k], place, left[k], bit)
            left[k] = [other for other in left[k] if other != bit]
    sums = [(q + hop(q, *zb[0])) * scale for q in sums]

    m = gather(after(mixing, theirs[0]), place, zb, zb)
    ma = gather(m[..., : br // 2, :], place, gb, up).reshape(G, Z, br // 2, bc)
    mb = gather(m[..., br // 2 :, :], place, gb, gb).reshape(G, Z, br // 2, bc)
    m_all = joined(core1, (ma, mb), (hop(ma, "gcol", 1), hop(mb, "gcol", 1)))
    acc = mixed((hh, hl), m_all)

    h_parts, mine, others = [], [], []
    for k, q in enumerate(sums):
        back = backs[k]
        h_parts.append(halves(q, place[zb[0]], 0)[0])
        row = gather(q, place, zb, zb[1:], zb[:1]).reshape(Z, b, bc).transpose(1, 0, 2).reshape(b, half)
        w = turned(core1, row, hop(row, "gcol", 1), m_all)
        w = gather(w, place, gb, back[:-1]).reshape(G * b // 2, half)
        got = hop(w, *back[-1])
        mine.append((w, hop(w, "gcol", 1)))
        others.append((got, hop(got, "gcol", 1)))

    part = None
    for j in range(2):
        part = less(at, acc, (ph, pl_), [w[j] for w in mine], j == 1, False, part)
    out = None
    for j in range(2):
        out = less(at, part, (ph, pl_), [w[j] for w in others], j == 1, True, out, True)

    h = jnp.concatenate(h_parts, 0)
    projected = lax.ppermute(h, "gcol", [(i, (i % 2) * Z + i // 2) for i in range(C)])
    return out, projected


def solution(mesh):
    return jax.shard_map(
        body,
        mesh=mesh,
        in_specs=(
            P(("grow", "gcol"), None),
            P(("grow", "gcol"), None),
            P(("grow", "gcol")),
            P("grow", "gcol"),
        ),
        out_specs=(P(("grow", "gcol"), None), P("grow", "gcol")),
        check_vma=False,
    )
```
